32 devices in a mesh: shard: 32 (over z, y, x, core).
Axes of the slice: x: 2, y: 2, z: 4, core: 2. Of those that a mesh axis runs over, the one named last changes fastest.
Arguments:
- tokens: bfloat16 [384, 197, 384], P('shard'), may hold values from -6 to 6
- cotangent: bfloat16 [384, 197, 384], P('shard'), may hold values from -6 to 6
- image_count: int32 [32], P('shard'), may hold values from 6 to 12, as said below
- attention_gain: bfloat16 [384], P('shard'), may hold values from 0.099609375 to 1.8984375
- attention_shift: bfloat16 [384], P('shard'), may hold values from -3 to 3
- input_weight: bfloat16 [384, 1152], P('shard'), may hold values from -0.3125 to 0.3125
- query_bias: bfloat16 [384], P('shard'), may hold values from -3 to 3
- value_bias: bfloat16 [384], P('shard'), may hold values from -3 to 3
- output_weight: bfloat16 [384, 384], P('shard'), may hold values from -1.25 to 1.25
- output_bias: bfloat16 [384], P('shard'), may hold values from -3 to 3
- feed_gain: bfloat16 [384], P('shard'), may hold values from 0.099609375 to 1.8984375
- feed_shift: bfloat16 [384], P('shard'), may hold values from -3 to 3
- up_weight: bfloat16 [384, 1536], P('shard'), may hold values from -0.3125 to 0.3125
- up_bias: bfloat16 [1536], P('shard'), may hold values from -3 to 3
- down_weight: bfloat16 [1536, 384], P('shard'), may hold values from -0.15625 to 0.15625
- down_bias: bfloat16 [384], P('shard'), may hold values from -3 to 3
Outputs:
- output: bfloat16 [384, 197, 384], P('shard')
- tokens_grad: bfloat16 [384, 197, 384], P('shard')
- attention_gain_grad: float32 [384], P('shard')
- attention_shift_grad: float32 [384], P('shard')
- input_weight_grad: float32 [384, 1152], P('shard')
- query_bias_grad: float32 [384], P('shard')
- value_bias_grad: float32 [384], P('shard')
- output_weight_grad: float32 [384, 384], P('shard')
- output_bias_grad: float32 [384], P('shard')
- feed_gain_grad: float32 [384], P('shard')
- feed_shift_grad: float32 [384], P('shard')
- up_weight_grad: float32 [384, 1536], P('shard')
- up_bias_grad: float32 [1536], P('shard')
- down_weight_grad: float32 [1536, 384], P('shard')
- down_bias_grad: float32 [384], P('shard')
The draws below stay inside these ranges and needn't reach their ends.
Inputs may be any that keep to these rules, and one draw needn't show every extreme that they name: Device i holds images in its first image_count[i] of 12 slots (rows 12 * i onward of tokens); its other slots are empty. Some device holds 12 images and some 12 // 2.
All inputs are finite; a program needn't handle non-finite values.
Results may differ from the reference program's by a relative error of at most 0.013.
The reference program's roundings to bfloat16 on the way count: a program that leaves them out, or rounds other values in their place, can miss the bound.
Values may be sent and summed in bfloat16 or wider, within the bound.
A program may use at most 128 MiB of HBM per device.

```python
import jax
import jax.numpy as jnp
from jax import lax

D = 384
HEADS = 6
HEAD_DIM = 64
FF = 1536
SEQ = 197
IMG_CAP = 12
SLOTS = 384
N_SHARD = 32


def draw_image_count(key, part):
    drawn = jax.random.randint(jax.random.fold_in(key, 1), (N_SHARD,), IMG_CAP // 2, IMG_CAP + 1)
    full_place = jax.random.randint(jax.random.fold_in(key, 2), (), 0, N_SHARD)
    offset = jax.random.randint(jax.random.fold_in(key, 3), (), 1, N_SHARD)
    half_place = (full_place + offset) % N_SHARD
    places = jnp.arange(N_SHARD)
    drawn = jnp.where(places == full_place, IMG_CAP, drawn)
    drawn = jnp.where(places == half_place, IMG_CAP // 2, drawn)
    return drawn.astype(jnp.int32)


def shard_levels(stream_key, shape, pieces, smallest, high):
    level, own = 1.0, jax.random.fold_in(stream_key, 6)
    for axis_at, parts in pieces:
        steps = jnp.exp(jax.random.uniform(jax.random.fold_in(own, axis_at), (parts,), jnp.float32, smallest / len(pieces), high / len(pieces)))
        level = level * jnp.repeat(steps, shape[axis_at] // parts).reshape([-1 if axis == axis_at else 1 for axis in range(len(shape))])
    return level


def scatter_about(rng, shape, scale, limit, split=(), held_as=jnp.bfloat16):
    entries = scale * jax.random.normal(rng, shape, jnp.float32)
    if split:
        entries = entries * shard_levels(rng, shape, split, -0.22, 0.18)
    return jnp.clip(entries, -limit, limit).astype(held_as)


def setup_inputs(seed: int = 0) -> dict:
    splits = jax.random.split(jax.random.key(seed), 17)
    tokens = scatter_about(splits[0], (SLOTS, SEQ, D), 1.0, 6.0, ((0, 32),))
    cotangent = scatter_about(splits[1], (SLOTS, SEQ, D), 1.0, 6.0, ((0, 32),))
    image_count = draw_image_count(jax.random.fold_in(splits[16], 71), 0)
    attention_gain = jnp.clip(1.0 + 0.18 * jax.random.normal(splits[3], (D,), jnp.float32), 0.099609375, 1.8984375).astype(jnp.bfloat16)
    attention_shift = scatter_about(splits[4], (D,), 0.5, 3.0, ((0, 32),))
    input_weight = scatter_about(splits[5], (D, 3 * D), D ** -0.5, 0.3125, ((0, 32),))
    query_bias = scatter_about(splits[6], (D,), 0.5, 3.0, ((0, 32),))
    value_bias = scatter_about(splits[7], (D,), 0.5, 3.0, ((0, 32),))
    output_weight = scatter_about(splits[8], (D, D), (D // 14) ** -0.5, 1.25, ((0, 32),))
    output_bias = scatter_about(splits[9], (D,), 0.5, 3.0, ((0, 32),))
    feed_gain = jnp.clip(1.0 + 0.18 * jax.random.normal(splits[10], (D,), jnp.float32), 0.099609375, 1.8984375).astype(jnp.bfloat16)
    feed_shift = scatter_about(splits[11], (D,), 0.5, 3.0, ((0, 32),))
    up_weight = scatter_about(splits[12], (D, FF), D ** -0.5, 0.3125, ((0, 32),))
    up_bias = scatter_about(splits[13], (FF,), 0.5, 3.0, ((0, 32),))
    down_weight = scatter_about(splits[14], (FF, D), FF ** -0.5, 0.15625, ((0, 32),))
    down_bias = scatter_about(splits[15], (D,), 0.5, 3.0, ((0, 32),))
    return {"tokens": tokens, "cotangent": cotangent, "image_count": image_count, "attention_gain": attention_gain, "attention_shift": attention_shift, "input_weight": input_weight, "query_bias": query_bias, "value_bias": value_bias, "output_weight": output_weight, "output_bias": output_bias, "feed_gain": feed_gain, "feed_shift": feed_shift, "up_weight": up_weight, "up_bias": up_bias, "down_weight": down_weight, "down_bias": down_bias}


@jax.custom_vjp
def low(v):
    return lax.optimization_barrier(v.astype(jnp.bfloat16)).astype(jnp.float32)

@jax.custom_vjp
def low_back(v):
    return v

def low_keep(v):
    return (low(v), None)

def low_pass(kept, grad):
    return (grad,)

def back_keep(v):
    return (v, None)

def back_low(kept, grad):
    return (low(grad),)
low.defvjp(low_keep, low_pass)
low_back.defvjp(back_keep, back_low)

def norm_rows(values, gain, shift):
    center = values - lax.optimization_barrier(jnp.mean(values, axis=-1, keepdims=True))
    spread = lax.optimization_barrier(jnp.mean(center * center, axis=-1, keepdims=True))
    return center * lax.rsqrt(spread + 1e-06) * gain + shift

def forward(block_in, params):
    attention_gain, attention_shift, input_weight, query_bias, value_bias, output_weight, output_bias, feed_gain, feed_shift, up_weight, up_bias, down_weight, down_bias = params
    highest = lax.Precision.HIGHEST
    images, seq_len, model_width = block_in.shape
    first = low(norm_rows(block_in, attention_gain, attention_shift))
    bias_full = jnp.concatenate([query_bias, jnp.zeros_like(query_bias), value_bias])
    mixed = jnp.einsum('bsd,de->bse', first, input_weight, precision=highest) + bias_full
    mixed = low_back(low(mixed))
    split_heads = mixed.reshape(images, seq_len, 3, HEADS, HEAD_DIM)
    query_rows = split_heads[:, :, 0]
    key_rows = split_heads[:, :, 1]
    value_rows = split_heads[:, :, 2]
    scores = jnp.einsum('bqhe,bkhe->bhqk', query_rows, key_rows, precision=highest) * HEAD_DIM ** (-0.5)
    scores = low_back(scores)
    exp_scores = jnp.exp(scores)
    probs = exp_scores / lax.optimization_barrier(jnp.sum(exp_scores, axis=-1, keepdims=True))
    context = jnp.einsum('bhqk,bkhe->bqhe', low(probs), value_rows, precision=highest)
    context = low_back(low(context)).reshape(images, seq_len, model_width)
    branch = jnp.einsum('bsd,de->bse', context, output_weight, precision=highest) + output_bias
    middle = block_in + low_back(branch)
    second = low(norm_rows(middle, feed_gain, feed_shift))
    hidden_pre = low_back(jnp.einsum('bsd,df->bsf', second, up_weight, precision=highest) + up_bias)
    hidden = low(jax.nn.gelu(hidden_pre, approximate=False))
    return middle + jnp.einsum('bsf,fd->bsd', hidden, down_weight, precision=highest) + down_bias

def reference(tokens, cotangent, image_count, attention_gain, attention_shift, input_weight, query_bias, value_bias, output_weight, output_bias, feed_gain, feed_shift, up_weight, up_bias, down_weight, down_bias):
    params = tuple((piece.astype(jnp.float32) for piece in (attention_gain, attention_shift, input_weight, query_bias, value_bias, output_weight, output_bias, feed_gain, feed_shift, up_weight, up_bias, down_weight, down_bias)))
    slot_tokens = tokens.reshape(N_SHARD, IMG_CAP, SEQ, D)
    slot_cot = cotangent.reshape(N_SHARD, IMG_CAP, SEQ, D)
    live_slots = jnp.arange(IMG_CAP, dtype=jnp.int32)[None, :] < image_count[:, None]

    def step(grad_total, item):
        block_in, cot_block, live_block = item
        result, pull = jax.vjp(forward, block_in.astype(jnp.float32), params)
        keep = live_block[:, None, None]
        grad_out = jnp.where(keep, cot_block.astype(result.dtype), 0.0)
        grad_in, grad_params = pull(grad_out)
        out_block = jnp.where(keep, result, 0.0).astype(jnp.bfloat16)
        return (jax.tree.map(jnp.add, grad_total, grad_params), (out_block, grad_in.astype(jnp.bfloat16)))
    zero_grads = jax.tree.map(jnp.zeros_like, params)
    grad_total, (outputs, grads_in) = lax.scan(step, zero_grads, (slot_tokens, slot_cot, live_slots))
    return (outputs.reshape(SLOTS, SEQ, D), grads_in.reshape(SLOTS, SEQ, D), grad_total[0], grad_total[1], grad_total[2], grad_total[3], grad_total[4], grad_total[5], grad_total[6], grad_total[7], grad_total[8], grad_total[9], grad_total[10], grad_total[11], grad_total[12])
```

```python
import functools
import math

import jax
import jax.numpy as jnp
from jax import lax
from jax.experimental import pallas as pl
from jax.experimental.pallas import tpu as pltpu
from jax.sharding import PartitionSpec as P

f32, bf16 = jnp.float32, jnp.bfloat16
HEAD_DIM = 64
EPS = 1e-06
LOG2E = math.log2(math.e)
SCALE = HEAD_DIM**-0.5
Z = 4
LANES = 128
AG, AS, QB, VB, OB, FG, FS, DB = range(8)


def nn(a, b):
    return jnp.dot(a, b, preferred_element_type=f32)


def nt(a, b):
    return lax.dot_general(a, b, (((1,), (1,)), ((), ())), preferred_element_type=f32)


def tn(a, b):
    return lax.dot_general(a, b, (((0,), (0,)), ((), ())), preferred_element_type=f32)


def normalize(x):
    c = x - jnp.mean(x, axis=-1, keepdims=True)
    inv = lax.rsqrt(jnp.mean(c * c, axis=-1, keepdims=True) + EPS)
    return c * inv, inv


def norm_back(w, n, inv):
    return inv * (w - jnp.mean(w, axis=-1, keepdims=True) - n * jnp.mean(w * n, axis=-1, keepdims=True))


def fold8(v):
    rows, cols = v.shape
    return jnp.sum(v.reshape(rows // 8, 8, cols), axis=0)


def pad_rows(v, rows):
    return jnp.concatenate([v, jnp.zeros((rows - v.shape[0], v.shape[1]), v.dtype)], axis=0)


class Place:
    def __init__(self, n):
        self.n, self.s = n, math.isqrt(n // (2 * Z))
        s = self.s
        me = lax.axis_index("shard")
        self.c = lax.rem(me, 2)
        q = lax.rem(lax.div(me, 2), s)
        p = lax.rem(lax.div(me, 2 * s), s)
        self.a = lax.div(me, 2 * s * s)
        self.f = p * (1 - self.c) + q * self.c
        self.g = q * (1 - self.c) + p * self.c

    def pq(self, f, g):
        return f * (1 - self.c) + g * self.c, g * (1 - self.c) + f * self.c

    def dev(self, a, f, g, c):
        p, q = self.pq(f, g)
        return ((a * self.s + p) * self.s + q) * 2 + c

    def around_a(self, k):
        return lax.rem(self.a + k, Z)

    def around_f(self, k):
        return lax.rem(self.f + k, self.s)

    def around_g(self, k):
        return lax.rem(self.g + k, self.s)

    def peers(self):
        s = self.s
        out = [self.dev(self.around_a(k), self.f, self.g, self.c) for k in range(1, Z)]
        out += [self.dev(self.a, self.around_f(k), self.g, self.c) for k in range(1, s)]
        out += [self.dev(self.a, self.f, self.around_g(k), self.c) for k in range(1, s)]
        p, q = self.pq(self.f, self.g)
        out.append(((self.a * s + p) * s + q) * 2 + 1 - self.c)
        return out


class Sems:
    def __init__(self, send, recv, local):
        self.send, self.recv, self.local, self.used, self.used_local = send, recv, local, 0, 0

    def take(self):
        self.used += 1
        return self.used - 1

    def take_local(self):
        self.used_local += 1
        return self.used_local - 1


class Step:
    def __init__(self, sems, moves):
        self.out, self.inn = [], []
        for src, dst, landing, dev in moves:
            k = sems.take()
            mk = functools.partial(
                pltpu.make_async_remote_copy,
                send_sem=sems.send.at[k],
                recv_sem=sems.recv.at[k],
                device_id=(dev,),
                device_id_type=pl.DeviceIdType.MESH,
            )
            self.out.append(mk(src_ref=src, dst_ref=dst))
            self.inn.append(mk(src_ref=landing, dst_ref=landing))

    def start(self):
        for m in self.out:
            m.start()

    def recv(self):
        for m in self.inn:
            m.wait_recv()

    def sent(self):
        for m in self.out:
            m.wait_send()


def gather_steps(pos, sems, g_ref, sources):
    s = pos.s
    p, q = pos.pq(pos.f, pos.g)

    def cols(lo, w):
        return (slice(None), pl.ds(lo, w))

    moves = []
    local = []
    for ref, lo, w in sources:
        k = sems.take_local()
        local.append(pltpu.make_async_copy(ref, g_ref.at[(pos.a, p, q, pos.c) + cols(lo, w)], sems.local.at[k]))
        for k in range(1, Z):
            there = g_ref.at[(pos.a, p, q, pos.c) + cols(lo, w)]
            here = g_ref.at[(pos.around_a(Z - k), p, q, pos.c) + cols(lo, w)]
            moves.append((ref, there, here, pos.dev(pos.around_a(k), pos.f, pos.g, pos.c)))
    one = Step(sems, moves)
    moves = []
    for k in range(1, s):
        pf, qf = pos.pq(pos.around_f(s - k), pos.g)
        there = g_ref.at[:, p, q, pos.c]
        moves.append((there, there, g_ref.at[:, pf, qf, pos.c], pos.dev(pos.a, pos.around_f(k), pos.g, pos.c)))
    two = Step(sems, moves)
    moves = []
    for k in range(1, s):
        for j in range(s):
            pj, qj = pos.pq(j, pos.g)
            pg, qg = pos.pq(j, pos.around_g(s - k))
            there = g_ref.at[:, pj, qj, pos.c]
            moves.append((there, there, g_ref.at[:, pg, qg, pos.c], pos.dev(pos.a, pos.f, pos.around_g(k), pos.c)))
    three = Step(sems, moves)
    there, here = g_ref.at[:, :, :, pos.c], g_ref.at[:, :, :, 1 - pos.c]
    four = Step(sems, [(there, there, here, ((pos.a * s + p) * s + q) * 2 + 1 - pos.c)])
    return local, [one, two, three, four]


class Scatter:
    def __init__(self, pos, sems, s_ref, r0, r1, r2, r3):
        self.pos, self.s_ref, self.r = pos, s_ref, (r0, r1, r2, r3)
        s, c = pos.s, pos.c
        p, q = pos.pq(pos.f, pos.g)
        steps = [Step(sems, [(s_ref.at[:, :, :, 1 - c], r0, r0, ((pos.a * s + p) * s + q) * 2 + 1 - c)])]
        moves = []
        for k in range(1, s):
            gk = pos.around_g(k)
            for j in range(s):
                pj, qj = pos.pq(j, gk)
                land = r1.at[k - 1, j]
                moves.append((s_ref.at[:, pj, qj, c], land, land, pos.dev(pos.a, pos.f, gk, c)))
        steps.append(Step(sems, moves))
        moves = []
        for k in range(1, s):
            fk = pos.around_f(k)
            pk, qk = pos.pq(fk, pos.g)
            land = r2.at[k - 1]
            moves.append((s_ref.at[:, pk, qk, c], land, land, pos.dev(pos.a, fk, pos.g, c)))
        steps.append(Step(sems, moves))
        moves = []
        for k in range(1, Z):
            ak = pos.around_a(k)
            land = r3.at[k - 1]
            moves.append((s_ref.at[ak, p, q, c], land, land, pos.dev(ak, pos.f, pos.g, c)))
        steps.append(Step(sems, moves))
        self.steps = steps

    def start(self):
        self.steps[0].start()

    def add(self, k):
        pos, s_ref = self.pos, self.s_ref
        s, c = pos.s, pos.c
        self.steps[k].recv()
        r = self.r[k]
        p, q = pos.pq(pos.f, pos.g)

        def one(at, terms):
            v = s_ref[at].astype(f32)
            for t in terms:
                v += t.astype(f32)
            s_ref[at] = v.astype(bf16)

        def slab(a, carry):
            if k == 0:
                for pp in range(s):
                    for qq in range(s):
                        one((a, pp, qq, c), [r[a, pp, qq]])
            elif k == 1:
                for j in range(s):
                    pj, qj = pos.pq(j, pos.g)
                    one((a, pj, qj, c), [r[m, j, a] for m in range(s - 1)])
            else:
                one((a, p, q, c), [r[m, a] for m in range(s - 1)])
            return carry

        lax.fori_loop(0, Z, slab, 0)
        self.steps[k + 1].start()

    def finish(self, out_ref):
        pos, r = self.pos, self.r[3]
        p, q = pos.pq(pos.f, pos.g)
        self.steps[3].recv()
        v = self.s_ref[pos.a, p, q, pos.c].astype(f32)
        for m in range(Z - 1):
            v += r[m].astype(f32)
        out_ref[...] = v
        for st in self.steps:
            st.sent()


def pieces(n):
    s = math.isqrt(n // (2 * Z))
    return [(a, p, q, c) for a in range(Z) for p in range(s) for q in range(s) for c in range(2)]


def repack(g_ref, w_ref, lo, width, n):
    at = pieces(n)
    rows = g_ref.shape[-2]
    per = math.lcm(rows, 16) // rows
    for b in range(n // per):
        for j in range(0, width, 384):
            w = min(384, width - j)
            parts = [g_ref[at[b * per + i] + (slice(None), slice(lo + j, lo + j + w))].astype(f32) for i in range(per)]
            w_ref[b * per * rows : (b + 1) * per * rows, j : j + w] = jnp.concatenate(parts, axis=0).astype(bf16)


def unpack(d_ref, s_ref, n):
    at = pieces(n)
    rows = s_ref.shape[-2]
    for k in range(n):
        s_ref[at[k]] = d_ref[k * rows : (k + 1) * rows, :].astype(bf16)


def kernel(n, grp, count_ref, tok_hbm, cot_hbm, win_hbm, wout_hbm, wup_hbm, wdn_hbm, v12_hbm, v48_hbm,
           out_hbm, tgrad_hbm, din_o, dout_o, dup_o, ddn_o,
           tok, cot, g_in, g_out, g_up, g_dn, w_in, w_out, w_up, vec, upb,
           firstT, kv_0, kv_1, mT_0, mT_1, vT_0, vT_1, p_0, p_1, cT_0, cT_1, mid_0, mid_1, n2_0, n2_1, inv_0, inv_1, sec, gl_s,
           hid, gp, dc_0, dc_1, dd_0, dd_1, ds_0, ds_1, gm_0, gm_1, acc, d_in, d_out, d_up, d_dn, d_upb,
           *rest):
    recvs, p_dn, (send_sem, recv_sem, local_sem, io_sem) = rest[:16], rest[16:-4], rest[-4:]
    images, seq, width = tok.shape
    ff = w_up.shape[1]
    heads = width // HEAD_DIM
    rp, qp = mid_0.shape[1], mT_0.shape[2]
    kv, mT, pr, cT, mid = (kv_0, kv_1), (mT_0, mT_1), (p_0, p_1), (cT_0, cT_1), (mid_0, mid_1)
    n2, inv2, vT = (n2_0, n2_1), (inv_0, inv_1), (vT_0, vT_1)
    dc, dd, ds, gm = (dc_0, dc_1), (dd_0, dd_1), (ds_0, ds_1), (gm_0, gm_1)
    live_count = count_ref[0]
    pos = Place(n)
    sems = Sems(send_sem, recv_sem, local_sem)
    whole = (ff // n) % 8 == 0
    g_dn6 = g_dn.reshape(Z, pos.s, pos.s, 2, ff // n, g_dn.shape[1]) if whole else p_dn[0]

    load_tok = pltpu.make_async_copy(tok_hbm, tok, io_sem.at[0])
    load_cot = pltpu.make_async_copy(cot_hbm, cot, io_sem.at[1])
    load_tok.start()
    load_cot.start()

    barrier = pltpu.get_barrier_semaphore()
    peers = pos.peers()
    for dev in peers:
        pl.semaphore_signal(barrier, inc=1, device_id=(dev,), device_id_type=pl.DeviceIdType.MESH)
    pl.semaphore_wait(barrier, len(peers))

    l_in, in_steps = gather_steps(pos, sems, g_in, [(win_hbm, 0, 3 * width), (v12_hbm, 3 * width, LANES)])
    l_out, out_steps = gather_steps(pos, sems, g_out, [(wout_hbm, 0, width)])
    l_up, up_steps = gather_steps(pos, sems, g_up, [(wup_hbm, 0, ff)])
    l_dn, dn_steps = gather_steps(pos, sems, g_dn6, [(wdn_hbm, 0, width), (v48_hbm, width, LANES)])
    for m in l_in + l_out + l_up + l_dn:
        m.start()
    in_steps[0].start()
    out_steps[0].start()
    for m in l_in:
        m.wait()
    in_steps[0].recv()
    in_steps[1].start()
    up_steps[0].start()
    dn_steps[0].start()
    for m in l_out:
        m.wait()
    out_steps[0].recv()
    out_steps[1].start()
    in_steps[1].recv()
    in_steps[2].start()
    out_steps[1].recv()
    out_steps[2].start()
    load_tok.wait()
    in_steps[2].recv()
    in_steps[3].start()
    out_steps[2].recv()
    out_steps[3].start()
    for m in l_up + l_dn:
        m.wait()
    for st in (up_steps, dn_steps):
        st[0].recv()
        st[1].start()
    in_steps[3].recv()
    repack(g_in, w_in, 0, w_in.shape[1], n)
    vec[...] = w_in[:, 3 * width :].astype(f32).T[:8, :]
    out_steps[3].recv()
    repack(g_out, w_out, 0, width, n)

    def row(k):
        return vec[k : k + 1, :]

    acc[...] = jnp.zeros_like(acc)
    d_in[...] = jnp.zeros_like(d_in)
    d_out[...] = jnp.zeros_like(d_out)
    d_up[...] = jnp.zeros_like(d_up)
    d_dn[...] = jnp.zeros_like(d_dn)
    d_upb[...] = jnp.zeros_like(d_upb)
    zero_head = jnp.zeros((HEAD_DIM, qp), bf16)

    def of_pair(h, v):
        return jnp.concatenate([v, zero_head] if h % 2 == 0 else [zero_head, v], axis=0)

    def head(h):
        return slice(HEAD_DIM * h, HEAD_DIM * (h + 1))

    def part(block, h):
        return slice(width * block + HEAD_DIM * h, width * block + HEAD_DIM * (h + 1))

    def pair(h, block=0):
        return slice(width * block + LANES * (h // 2), width * block + LANES * (h // 2 + 1))

    def tokens(i):
        return pad_rows(tok[i].astype(f32), rp)

    def a_first(i, b, u):
        x, _ = normalize(tokens(i))
        first = (x * row(AG) + row(AS)).astype(bf16)
        firstT[i, :width, :] = pad_rows(first, qp).T
        firstT[i, width:, :] = jnp.ones((firstT.shape[1] - width, qp), bf16)
        return first

    def a_mixed(first, b, u):
        bias = jnp.concatenate([row(QB), jnp.zeros((1, width), f32), row(VB)], axis=1)
        mixed = (nn(first, w_in[:, : 3 * width]) + bias).astype(bf16)
        kv[u][b] = mixed[:, width:]
        turned = pad_rows(mixed, qp).T
        mT[u][b] = turned[: 2 * width, :]
        vT[u][...] = turned[2 * width :, :]

    def a_probs(b, u):
        key_row = lax.broadcasted_iota(jnp.int32, (rp, qp), 0)
        for h in range(heads):
            s = nn(kv[u][b, :, pair(h)], of_pair(h, mT[u][b, part(0, h), :]))
            e = jnp.where(key_row < seq, jnp.exp2(s * (SCALE * LOG2E)), 0.0)
            pr[u][b, h] = (e * (1.0 / jnp.sum(e, axis=0, keepdims=True))).astype(bf16)

    def a_context(b, u):
        for h in range(heads):
            cT[u][b, head(h), :] = nn(vT[u][head(h), :rp], pr[u][b, h]).astype(bf16)

    def a_middle(i, b, u):
        mid[u][b] = tokens(i) + tn(cT[u][b], w_out[...])[:rp] + row(OB)

    def gather_tick(t):
        for k, (last, nxt) in enumerate(((1, 2), (2, 3))):
            @pl.when(t == 1 + 2 * k)
            def _():
                for st in (up_steps, dn_steps):
                    st[last].recv()
                    st[nxt].start()

    def a_body(i, b, u, i1, b1, u1, i2, b2, u2):
        first = a_first(i, b, u)
        a_probs(b1, u1)
        a_mixed(first, b, u)
        if i2 is not None:
            a_middle(i2, b2, u2)
        a_context(b1, u1)

    a_mixed(a_first(0, 0, 0), 0, 0)
    a_body(1, 0, 1, 0, 0, 0, None, None, None)

    def a_pair(t, carry):
        gather_tick(t)
        i = 2 * t + 2
        a_body(i, t + 1, 0, i - 1, t, 1, i - 2, t, 0)
        a_body(i + 1, t + 1, 1, i, t + 1, 0, i - 1, t, 1)
        return carry

    half = images // 2
    lax.fori_loop(0, half - 1, a_pair, 0)
    a_probs(half - 1, 1)
    a_middle(images - 2, half - 1, 0)
    a_context(half - 1, 1)
    a_middle(images - 1, half - 1, 1)

    for st in (up_steps, dn_steps):
        st[3].recv()
    repack(g_up, w_up, 0, ff, n)
    if not whole:
        repack(g_dn6, g_dn, 0, g_dn.shape[1], n)
    upb[...] = g_dn[:, width:].astype(f32).T[:8, :]
    load_cot.wait()
    for steps in (in_steps, out_steps, up_steps, dn_steps):
        for st in steps:
            st.sent()

    def rows(k):
        return pl.ds(pl.multiple_of(k * rp, 16), rp)

    def b_norm(i, b, u, k):
        n2[u][...], inv2[u][...] = normalize(mid[u][b])
        sec[rows(k), :] = (n2[u][...] * row(FG) + row(FS)).astype(bf16)
        gl_s[rows(k), :] = jnp.where(i < live_count, pad_rows(cot[i].astype(f32), rp), 0.0).astype(bf16)

    def b_hidden(k):
        second, grad = sec[rows(k), :], gl_s[rows(k), :]
        for j in range(ff // 256):
            cols = slice(256 * j, 256 * (j + 1))
            v = nn(second, w_up[:, cols]) + upb[0:1, cols]
            gh = nt(grad, g_dn[cols, :width])
            phi = 0.5 + 0.5 * lax.erf(v * math.sqrt(0.5))
            dens = jnp.exp2(v * v * (-0.5 * LOG2E))
            hid[rows(k), cols] = (v * phi).astype(bf16)
            gp[rows(k), cols] = (gh * (phi + v * dens * (1 / math.sqrt(2 * math.pi)))).astype(bf16)

    def b_out(i, b, u, k):
        y = nn(hid[rows(k), :], g_dn[:, :width]) + mid[u][b] + row(DB)
        cot[i] = jnp.where(i < live_count, y, 0.0).astype(bf16)[:seq]

    def b_back(b, u, k):
        gs = nt(gp[rows(k), :], w_up[...])
        grad, normed = gl_s[rows(k), :].astype(f32), n2[u][...]
        gmid = grad + norm_back(gs * row(FG), normed, inv2[u][...])
        mid[u][b] = gmid
        acc[8 * DB : 8 * DB + 8, :] += fold8(grad)
        acc[8 * FG : 8 * FG + 8, :] += fold8(gs * normed)
        acc[8 * FS : 8 * FS + 8, :] += fold8(gs)
        acc[8 * OB : 8 * OB + 8, :] += fold8(gmid.astype(bf16).astype(f32))

    def b_outw(b, u):
        d_out[...] += nn(cT[u][b][:, :rp], mid[u][b].astype(bf16))

    def b_body(i, b, u, b1, u1, k):
        b_out(i - 1, b1, u1, k - 1)
        b_back(b1, u1, k - 1)
        b_norm(i, b, u, k)
        b_hidden(k)
        b_outw(b1, u1)

    def b_group(t, carry):
        i0, b0 = t * grp, t * (grp // 2)
        b_norm(i0, b0, 0, 0)
        b_hidden(0)

        def b_pair(r, c):
            i = i0 + 2 * r + 1
            b_body(i, b0 + r, 1, b0 + r, 0, 2 * r + 1)
            b_body(i + 1, b0 + r + 1, 0, b0 + r, 1, 2 * r + 2)
            return c

        lax.fori_loop(0, grp // 2 - 1, b_pair, 0)
        be = b0 + grp // 2 - 1
        b_body(i0 + grp - 1, be, 1, be, 0, grp - 1)
        b_out(i0 + grp - 1, be, 1, grp - 1)
        b_back(be, 1, grp - 1)
        b_outw(be, 1)

        def b_weights(j, c):
            cols = pl.ds(pl.multiple_of(j * 512, 512), 512)
            d_up[:, cols] += tn(sec[...], gp[:, cols])
            d_dn[:, cols] += tn(gl_s[...], hid[:, cols])
            d_upb[:, cols] += nn(jnp.ones((d_upb.shape[0], gp.shape[0]), bf16), gp[:, cols])
            return c

        lax.fori_loop(0, ff // 512, b_weights, 0)
        return carry

    lax.fori_loop(0, images // grp, b_group, 0)
    store_out = pltpu.make_async_copy(cot, out_hbm, io_sem.at[1])
    store_out.start()

    rs_in, rs_out, rs_up, rs_dn = [
        Scatter(pos, sems, ref, *recvs[4 * k : 4 * k + 4]) for k, ref in enumerate((g_in, g_out, g_up, g_dn6))
    ]
    unpack(d_up, g_up, n)
    rs_up.start()
    for j in range(0, ff, LANES):
        block = jnp.concatenate([d_dn[:, j : j + LANES], pad_rows(d_upb[:8, j : j + LANES], LANES)], axis=0)
        g_dn[j : j + LANES, :] = block.T.astype(bf16)
    if not whole:
        unpack(g_dn, g_dn6, n)
    rs_dn.start()
    unpack(d_out, g_out, n)
    rs_out.start()
    early = (rs_up, rs_dn, rs_out)

    def c_context(b, u):
        g = nt(w_out[...], pad_rows(mid[u][b].astype(bf16), qp)).astype(bf16)
        dc[u][...] = g
        prod = g.astype(f32) * cT[u][b].astype(f32)
        sums = [jnp.sum(prod[head(h), :], axis=0, keepdims=True) for h in range(heads)]
        dd[u][...] = jnp.concatenate(sums + [jnp.zeros((8 - heads, qp), f32)], axis=0)

    def c_scores(b, u):
        for h in range(heads):
            dp = nn(kv[u][b, :, pair(h, 1)], of_pair(h, dc[u][head(h), :]))
            ds[u][h] = (pr[u][b, h].astype(f32) * (dp - dd[u][h : h + 1, :])).astype(bf16)

    def c_value(b, u):
        for h in range(heads):
            gm[u][part(2, h), :rp] = nt(dc[u][head(h), :], pr[u][b, h]).astype(bf16)

    def c_query_key(b, u):
        for h in range(heads):
            g = ds[u][h]
            gm[u][part(0, h), :] = (nn(mT[u][b, part(1, h), :rp], g) * SCALE).astype(bf16)
            gm[u][part(1, h), :rp] = (nt(mT[u][b, part(0, h), :], g) * SCALE).astype(bf16)

    def c_inw(i, u):
        d_in[:, : 3 * width] += nt(firstT[i][:, :rp], gm[u][:, :rp])

    def c_first(i, b, u):
        gf = nn(w_in[:, : 3 * width], gm[u][...]).T[:rp]
        normed, inv = normalize(tokens(i))
        acc[8 * AG : 8 * AG + 8, :] += fold8(gf * normed)
        acc[8 * AS : 8 * AS + 8, :] += fold8(gf)
        tok[i] = (mid[u][b] + norm_back(gf * row(AG), normed, inv)).astype(bf16)[:seq]

    def scatter_tick(t):
        for k in range(3):
            @pl.when(t == 1 + k)
            def _():
                for rs in early:
                    rs.add(k)

    def c_body(b, u, b1, u1, i2, b2, u2):
        if i2 is not None:
            c_inw(i2, u2)
        c_scores(b1, u1)
        if i2 is not None:
            c_first(i2, b2, u2)
        c_value(b1, u1)
        if b is not None:
            c_context(b, u)
        c_query_key(b1, u1)

    c_context(0, 0)
    c_body(0, 1, 0, 0, None, None, None)

    def c_pair(t, carry):
        scatter_tick(t)
        i = 2 * t + 2
        c_body(t + 1, 0, t, 1, i - 2, t, 0)
        c_body(t + 1, 1, t + 1, 0, i - 1, t, 1)
        return carry

    lax.fori_loop(0, half - 1, c_pair, 0)
    c_body(None, None, half - 1, 1, images - 2, half - 1, 0)
    c_inw(images - 1, 1)
    sums = {QB: d_in[width : width + 1, :width], VB: d_in[width : width + 1, 2 * width : 3 * width]}

    def c_vectors():
        table = []
        for k in range(8):
            table.append(sums[k] if k in sums else jnp.sum(acc[8 * k : 8 * k + 8, :], axis=0, keepdims=True))
        d_in[:width, 3 * width :] = pad_rows(jnp.concatenate(table, axis=0), LANES).T

    c_first(images - 1, half - 1, 1)
    store_tgrad = pltpu.make_async_copy(tok, tgrad_hbm, io_sem.at[0])
    store_tgrad.start()
    c_vectors()
    unpack(d_in, g_in, n)
    rs_in.start()
    rs_up.finish(dup_o)
    rs_dn.finish(ddn_o)
    rs_out.finish(dout_o)
    for k in range(3):
        rs_in.add(k)
    rs_in.finish(din_o)
    store_out.wait()
    store_tgrad.wait()


def build(n, images, seq, width, ff):
    heads = width // HEAD_DIM
    rp, qp = -(-seq // 16) * 16, -(-seq // LANES) * LANES
    s = math.isqrt(n // (2 * Z))
    grp = 6 if n <= 32 else 2
    half = images // 2
    rows, rows_ff = width // n, ff // n

    def vm(*shape, dtype=bf16):
        return pltpu.VMEM(shape, dtype)

    def twice(*shape, dtype=bf16):
        return [vm(*shape, dtype=dtype)] * 2

    lead = (Z, s, s, 2)
    chunks = ((rows, 3 * width + LANES), (rows, width), (rows, ff), (rows_ff, width + LANES))
    recvs = []
    for rc in chunks:
        recvs += [vm(Z, s, s, *rc), vm(s - 1, s, Z, *rc), vm(s - 1, Z, *rc), vm(Z - 1, *rc)]
    remote = 2 * 4 * (Z - 1 + (s - 1) + (s - 1) * s + 1) + 2 * (Z - 1)
    scratch = [
        vm(images, seq, width),
        vm(images, seq, width),
        vm(*lead, *chunks[0]),
        vm(*lead, *chunks[1]),
        vm(*lead, *chunks[2]),
        vm(ff, width + LANES),
        vm(width, 3 * width + LANES),
        vm(width, width),
        vm(width, ff),
        vm(8, width, dtype=f32),
        vm(8, ff, dtype=f32),
        vm(images, width + 16, qp),
        *twice(half, rp, 2 * width),
        *twice(half, 2 * width, qp),
        *twice(width, qp),
        *twice(half, heads, rp, qp),
        *twice(half, width, qp),
        *twice(half, rp, width, dtype=f32),
        *twice(rp, width, dtype=f32),
        *twice(rp, 1, dtype=f32),
        vm(grp * rp, width),
        vm(grp * rp, width),
        vm(grp * rp, ff),
        vm(grp * rp, ff),
        *twice(width, qp),
        *twice(8, qp, dtype=f32),
        *twice(heads, rp, qp),
        *twice(3 * width, qp),
        vm(64, width, dtype=f32),
        vm(width + 16, 3 * width + LANES, dtype=f32),
        vm(width, width, dtype=f32),
        vm(width, ff, dtype=f32),
        vm(width, ff, dtype=f32),
        vm(16, ff, dtype=f32),
        *recvs,
        *([] if rows_ff % 8 == 0 else [vm(*lead, *chunks[3])]),
        pltpu.SemaphoreType.DMA((remote,)),
        pltpu.SemaphoreType.DMA((remote,)),
        pltpu.SemaphoreType.DMA((6,)),
        pltpu.SemaphoreType.DMA((2,)),
    ]
    anywhere = pl.BlockSpec(memory_space=pl.ANY)
    vmem = pl.BlockSpec(memory_space=pltpu.VMEM)
    shape = jax.ShapeDtypeStruct
    return pl.pallas_call(
        functools.partial(kernel, n, grp),
        in_specs=[pl.BlockSpec(memory_space=pltpu.SMEM)] + [anywhere] * 8,
        out_specs=[anywhere] * 2 + [vmem] * 4,
        out_shape=[shape((images, seq, width), bf16)] * 2 + [shape(rc, f32) for rc in chunks],
        scratch_shapes=scratch,
        compiler_params=pltpu.CompilerParams(
            collective_id=0, has_side_effects=True, vmem_limit_bytes=67043328
        ),
        name="encoder",
    )


def shards(
    tokens, cotangent, image_count, attention_gain, attention_shift, input_weight, query_bias, value_bias,
    output_weight, output_bias, feed_gain, feed_shift, up_weight, up_bias, down_weight, down_bias, *, n,
):
    images, seq, width = tokens.shape
    ff = up_weight.shape[1]
    vectors = (attention_gain, attention_shift, query_bias, value_bias, output_bias, feed_gain, feed_shift, down_bias)
    v12 = jnp.pad(jnp.stack(vectors, axis=1), ((0, 0), (0, LANES - 8)))
    v48 = jnp.pad(up_bias[:, None], ((0, 0), (0, LANES - 1)))
    out, tgrad, d_in, d_out, d_up, d_dn = build(n, images, seq, width, ff)(
        image_count, tokens, cotangent, input_weight, output_weight, up_weight, down_weight, v12, v48
    )
    col = [d_in[:, 3 * width + k] for k in range(8)]
    return (
        out, tgrad, col[AG], col[AS], d_in[:, : 3 * width], col[QB], col[VB], d_out, col[OB], col[FG], col[FS],
        d_up, d_dn[:, width], d_dn[:, :width], col[DB],
    )


def solution(mesh):
    n = mesh.shape["shard"]
    cube, flat, mat = P("shard", None, None), P("shard"), P("shard", None)
    return jax.shard_map(
        functools.partial(shards, n=n),
        mesh=mesh,
        in_specs=(cube, cube, flat, flat, flat, mat, flat, flat, mat, flat, flat, flat, mat, flat, mat, flat),
        out_specs=(cube, cube, flat, flat, mat, flat, flat, mat, flat, flat, flat, mat, flat, mat, flat),
        check_vma=False,
    )
```
